512 devices in a mesh: gx: 8 (over x, y_hi), gy: 8 (over z), gz: 8 (over y_lo, core).
Axes of the slice: x: 4, y: 8 (y_hi: 2, y_lo: 4; y = y_hi * 4 + y_lo), z: 8, core: 2. Of those that a mesh axis runs over, the one named last changes fastest.
Arguments:
- correlators: bfloat16 [32, 64, 64, 64, 128], P(None, 'gx', 'gy', 'gz'), may hold values from -6 to 6
- momenta: int32 [125, 3], replicated, may hold values from -32 to 31
- source_channel: int32 [64], replicated, may hold values from 0 to 63
- phase_code: int32 [64], replicated, may hold values from 0 to 3
Outputs:
- projected: float32 [32, 125, 128], P('gx', None, ('gy', 'gz'))
The draws below stay inside these ranges and needn't reach their ends.
All inputs are finite; a program needn't handle non-finite values.
Results may differ from the reference program's by a relative error of at most 0.002.
Values sent between devices are 32-bit elements; how exact they have to be, the bound alone decides.
A program may use at most 64 MiB of HBM per device.

```python
import math
import jax
import jax.numpy as jnp
from jax import lax

CH = 64
MOM = 125
TW = 32
NX = 64
NY = 64
NZ = 64


def set_ends(drawn, key, least, top_value):
    index_at = [jax.random.randint(jax.random.fold_in(key, axis), (), 0, length) for axis, length in enumerate(drawn.shape)]
    main_axis = drawn.shape.index(max(drawn.shape))
    beside = index_at[:main_axis] + [(index_at[main_axis] + 1) % drawn.shape[main_axis]] + index_at[main_axis + 1:]
    return drawn.at[tuple(index_at)].set(least).at[tuple(beside)].set(top_value)


def shard_levels(own_key, shape, shards, low, top_value):
    loudness, own = 1.0, jax.random.fold_in(own_key, 6)
    for dim, blocks in shards:
        steps = jnp.exp(jax.random.uniform(jax.random.fold_in(own, dim), (blocks,), jnp.float32, low / len(shards), top_value / len(shards)))
        loudness = loudness * jnp.repeat(steps, shape[dim] // blocks).reshape([-1 if axis == dim else 1 for axis in range(len(shape))])
    return loudness


def normal_values(own_key, shape, scale, limit, split=(), kind=jnp.bfloat16):
    result = jax.random.normal(own_key, shape, jnp.float32) * scale
    if len(split) > 0:
        result = shard_levels(own_key, shape, split, -0.22, 0.18) * result
    return jnp.clip(result, min=-limit, max=limit).astype(kind)


def setup_inputs(seed: int = 0) -> dict:
    key_of = jax.random.split(jax.random.key(seed), 5)
    return {
        "correlators": normal_values(key_of[0], (TW, NX, NY, NZ, 2 * CH), 1.0, 6.0, ((1, 8), (2, 8), (3, 8))),
        "momenta": set_ends(jax.random.randint(key_of[1], (MOM, 3), 0 - min(min(NX, NY), NZ) // 2, min(min(NX, NY), NZ) // 2), jax.random.fold_in(key_of[1], 1), 0 - min(min(NX, NY), NZ) // 2, (min(min(NX, NY), NZ) // 2) - 1).astype(jnp.int32),
        "source_channel": set_ends(jax.random.randint(key_of[2], (CH,), 0, CH), jax.random.fold_in(key_of[2], 1), 0, CH - 1).astype(jnp.int32),
        "phase_code": set_ends(jax.random.randint(key_of[3], (CH,), 0, 4), jax.random.fold_in(key_of[3], 1), 0, 3).astype(jnp.int32),
    }


def axis_fraction(values, coords, extent):
    return jnp.mod(values[:, None] * coords[None, :], extent).astype(jnp.float32) / extent

def phase_table(momenta, coord_x, coord_y, coord_z, size_x, size_y, size_z):
    frac_x = axis_fraction(momenta[:, 0], coord_x, size_x)
    frac_y = axis_fraction(momenta[:, 1], coord_y, size_y)
    frac_z = axis_fraction(momenta[:, 2], coord_z, size_z)
    summed = frac_x[:, :, None, None] + frac_y[:, None, :, None]
    summed = summed + frac_z[:, None, None, :]
    angles = (summed * (2.0 * math.pi)).reshape(momenta.shape[0], -1)
    return jnp.concatenate([jnp.cos(angles), jnp.sin(angles)], axis=0).astype(jnp.bfloat16)

def channel_signs(phase_code):
    real_sign = jnp.where(phase_code == 0, 1.0, jnp.where(phase_code == 2, -1.0, 0.0)).astype(jnp.float32)
    imag_sign = jnp.where(phase_code == 1, 1.0, jnp.where(phase_code == 3, -1.0, 0.0)).astype(jnp.float32)
    return (real_sign, imag_sign)

def reference(correlators, momenta, source_channel, phase_code):
    channels = correlators.shape[-1] // 2
    moment_count = momenta.shape[0]
    phases = phase_table(momenta, jnp.arange(NX, dtype=jnp.int32), jnp.arange(NY, dtype=jnp.int32), jnp.arange(NZ, dtype=jnp.int32), NX, NY, NZ).astype(jnp.float32)
    real_sign, imag_sign = channel_signs(phase_code)
    norm_factor = 1.0 / math.sqrt(NX * NY * NZ)

    def project(one_slice):
        values = one_slice.reshape(-1, 2 * channels).astype(jnp.float32)
        real_src = jnp.take(values[:, :channels], source_channel, axis=1)
        imag_src = jnp.take(values[:, channels:], source_channel, axis=1)
        real_mix = real_sign[None, :] * real_src - imag_sign[None, :] * imag_src
        imag_mix = imag_sign[None, :] * real_src + real_sign[None, :] * imag_src
        mixed = jnp.concatenate([real_mix, imag_mix], axis=1).astype(jnp.bfloat16)
        mixed = lax.optimization_barrier(mixed).astype(jnp.float32)
        product = jnp.dot(phases, mixed, preferred_element_type=jnp.float32)
        cos_part = product[:moment_count]
        sin_part = product[moment_count:]
        real_out = cos_part[:, :channels] + sin_part[:, channels:]
        imag_out = cos_part[:, channels:] - sin_part[:, :channels]
        return jnp.concatenate([real_out, imag_out], axis=1) * norm_factor
    return lax.map(project, correlators)
```

```python
import math

import jax
import jax.numpy as jnp
from jax import lax
from jax.experimental import pallas as pl
from jax.experimental.pallas import tpu as pltpu
from jax.sharding import PartitionSpec as P

MESH = pl.DeviceIdType.MESH
ORDER = (2, 1, 3, 0)
SLOT = {k: i for i, k in enumerate(ORDER)}
NT = (((1,), (1,)), ((), ()))


def phase_weights(mom_ref, padded, weights):
    padded[...] = jnp.zeros_like(padded)
    padded[:, 0:125] = mom_ref[...]
    own = lax.broadcasted_iota(jnp.int32, (8, 128), 0)
    cos, sin = [], []
    for row, axis in enumerate(("gx", "gy", "gz")):
        turns = (padded[row : row + 1, :] * (own + 8 * lax.axis_index(axis))) & 63
        angle = turns.astype(jnp.float32) * (2.0 * math.pi / 64.0)
        cos.append(jnp.cos(angle))
        sin.append(jnp.sin(angle))
    cos_yz = jnp.concatenate([cos[1][y : y + 1] * cos[2] - sin[1][y : y + 1] * sin[2] for y in range(8)], axis=0)
    sin_yz = jnp.concatenate([sin[1][y : y + 1] * cos[2] + cos[1][y : y + 1] * sin[2] for y in range(8)], axis=0)
    for x in range(8):
        c = (cos[0][x : x + 1] * cos_yz - sin[0][x : x + 1] * sin_yz).astype(jnp.bfloat16)
        s = (sin[0][x : x + 1] * cos_yz + cos[0][x : x + 1] * sin_yz).astype(jnp.bfloat16)
        rows, more = pl.ds(64 * x, 64), pl.ds(512 + 64 * x, 64)
        weights[rows, 0:128] = c
        weights[rows, 128:256] = -s
        weights[more, 0:128] = s
        weights[more, 128:256] = c


def mixing_rows(src_ref, code_ref, core):
    raw = lax.broadcasted_iota(jnp.int32, (128, 64), 0)
    src, code = src_ref[...], code_ref[...]
    one, none = jnp.float32(1.0), jnp.float32(0.0)
    real_sign = jnp.where(code == 0, one, jnp.where(code == 2, -one, none))
    imag_sign = jnp.where(code == 1, one, jnp.where(code == 3, -one, none))
    from_real = jnp.where(raw == src, one, none)
    from_imag = jnp.where(raw == src + 64, one, none)
    to_real = from_real * real_sign - from_imag * imag_sign
    to_imag = from_real * imag_sign + from_imag * real_sign
    row = lax.broadcasted_iota(jnp.int32, (64, 64), 0)
    channel = lax.broadcasted_iota(jnp.int32, (64, 64), 1)
    outer, inner, last = (row >> 3) & 3, (row >> 1) & 3, row & 1
    side = (row >> 5) ^ core
    result = []
    for z, y in ((outer, inner), (inner, outer)):
        chosen = jnp.where(channel == z * 16 + y * 4 + side * 2 + last, one, none).astype(jnp.bfloat16)
        parts = [
            lax.dot_general(chosen, part.astype(jnp.bfloat16), NT, preferred_element_type=jnp.float32)
            for part in (to_real, to_imag)
        ]
        result.append(jnp.concatenate(parts, axis=0).astype(jnp.bfloat16))
    return result


def kernel(corr, mom_ref, src_ref, code_ref, out_ref, inbuf, padded, weights, left, own, give, take,
           z1, z1r, z2, z2r, y1, y1r, y2, y2r, a1, a1r, a2, a2r, b1, b1r, b2, b2r, p3, p3r,
           in_sem, core_send, core_recv, send_sem, recv_sem):
    gx, gy, gz = lax.axis_index("gx"), lax.axis_index("gy"), lax.axis_index("gz")
    x, y_hi, z, y_lo, core = gx // 2, gx % 2, gy, gz // 2, gz % 2
    y = y_hi * 4 + y_lo

    def at_x(k):
        return (((x + k) % 4) * 2 + y_hi, gy, gz)

    def at_y(k):
        to = (y + k) % 8
        return ((x * 2 + to // 4), gy, (to % 4) * 2 + core)

    def at_z(k):
        return (gx, (z + k) % 8, gz)

    partner = (gx, gy, y_lo * 2 + (1 - core))

    barrier = pltpu.get_barrier_semaphore()
    peers = [partner] + [at_x(k) for k in range(1, 4)]
    peers += [at_y(k) for k in range(1, 8)] + [at_z(k) for k in range(1, 8)]
    for peer in peers:
        pl.semaphore_signal(barrier, inc=1, device_id=peer, device_id_type=MESH)

    loads = []
    for i, k in enumerate(ORDER):
        rows = pl.ds(pl.multiple_of(((x + k) % 4) * 4096, 4096), 4096)
        load = pltpu.make_async_copy(corr.at[rows], inbuf.at[i], in_sem.at[i])
        load.start()
        loads.append(load)

    phase_weights(mom_ref, padded, weights)
    mix_zy, mix_yz = mixing_rows(src_ref, code_ref, core)

    sent = []

    def send(src, dst, channel, to):
        copy = pltpu.make_async_remote_copy(
            src_ref=src, dst_ref=dst, send_sem=send_sem.at[channel], recv_sem=recv_sem.at[channel],
            device_id=to, device_id_type=MESH)
        copy.start()

    def arrived(ref, channel):
        pltpu.make_async_copy(ref, ref, recv_sem.at[channel]).wait()

    def departed(ref, channel):
        pltpu.make_async_copy(ref, ref, send_sem.at[channel]).wait()

    swaps = []

    def compute(i):
        loads[i].wait()
        for t in range(8):
            mix = mix_zy if t % 4 in (0, 3) else mix_yz
            mixed = lax.dot_general(
                mix, inbuf[i, t * 512 : (t + 1) * 512, :], NT, preferred_element_type=jnp.float32
            ).astype(jnp.bfloat16)
            left[t * 64 : (t + 1) * 64, 0:512] = mixed[0:64]
            left[t * 64 : (t + 1) * 64, 512:1024] = mixed[64:128]
        product = jnp.dot(left[...], weights[...], preferred_element_type=jnp.float32)
        for t in range(8):
            for half in range(2):
                lanes = slice(half * 128, half * 128 + 128)
                own[i, t, half] = product[t * 64 : t * 64 + 32, lanes]
                give[i, t, half] = product[t * 64 + 32 : t * 64 + 64, lanes]
        if i == 0:
            pl.semaphore_wait(barrier, len(peers))
        swap = pltpu.make_async_remote_copy(
            src_ref=give.at[i], dst_ref=take.at[i], send_sem=core_send.at[i], recv_sem=core_recv.at[i],
            device_id=partner, device_id_type=MESH)
        swap.start()
        swaps.append(swap)

    def first_phase(i):
        swaps[i].wait_recv()
        for yh in range(2):
            for half in range(2):
                for tt in range(4):
                    t = yh * 4 + tt
                    value = (own[i, t, half] + take[i, t, half]).reshape(4, 8, 128)
                    if tt == 0:
                        for q in range(4):
                            z1[half * 4 + q, i, yh] = value[q]
                    elif tt == 1:
                        for q in range(4):
                            y1[yh * 4 + q, i, half] = value[q]
                    elif tt == 2:
                        for q in range(4):
                            a1[i, yh * 4 + q, half] = value[q]
                    else:
                        for q in range(4):
                            b1[i, half * 4 + q, yh] = value[q]
        k = ORDER[i]
        if k != 0:
            send(a1.at[i], a1r.at[k - 1], 0, at_x(k))
            send(b1.at[i], b1r.at[k - 1], 1, at_x(k))
        for k in (4, 3, 5, 2, 6, 1, 7):
            send(z1.at[(z + k) % 8, i], z1r.at[k - 1, i], 2, at_z(k))
            send(y1.at[(y + k) % 8, i], y1r.at[k - 1, i], 3, at_y(k))

    for i in range(4):
        compute(i)
        if i >= 1:
            first_phase(i - 1)
    first_phase(3)

    arrived(a1r, 0)
    a2[...] = a1[SLOT[0]] + a1r[0] + a1r[1] + a1r[2]
    for k in (4, 3, 5, 2, 6, 1, 7):
        send(a2.at[(y + k) % 8], a2r.at[k - 1], 4, at_y(k))
    arrived(b1r, 1)
    b2[...] = b1[SLOT[0]] + b1r[0] + b1r[1] + b1r[2]
    for k in (4, 3, 5, 2, 6, 1, 7):
        send(b2.at[(z + k) % 8], b2r.at[k - 1], 5, at_z(k))
    arrived(z1r, 2)
    z2[...] = z1[z] + ((z1r[0] + z1r[1]) + (z1r[2] + z1r[3])) + ((z1r[4] + z1r[5]) + z1r[6])
    for k in (2, 1, 3):
        send(z2.at[SLOT[k]], z2r.at[k - 1], 6, at_x(k))
    arrived(y1r, 3)
    y2[...] = y1[y] + ((y1r[0] + y1r[1]) + (y1r[2] + y1r[3])) + ((y1r[4] + y1r[5]) + y1r[6])
    for k in (2, 1, 3):
        send(y2.at[SLOT[k]], y2r.at[k - 1], 7, at_x(k))

    def spread(stream, value, at, mine):
        rows = value.reshape(16, 128)
        for q in range(8):
            p3[stream, q] = rows[2 * q : 2 * q + 2]
        for k in (4, 3, 5, 2, 6, 1, 7):
            send(p3.at[stream, (mine + k) % 8], p3r.at[stream, k - 1], 8 + stream, at(k))

    arrived(z2r, 6)
    spread(0, z2[SLOT[0]] + z2r[0] + z2r[1] + z2r[2], at_y, y)
    arrived(y2r, 7)
    spread(1, y2[SLOT[0]] + y2r[0] + y2r[1] + y2r[2], at_z, z)
    arrived(a2r, 4)
    spread(2, a2[y] + ((a2r[0] + a2r[1]) + (a2r[2] + a2r[3])) + ((a2r[4] + a2r[5]) + a2r[6]), at_z, z)
    arrived(b2r, 5)
    spread(3, b2[z] + ((b2r[0] + b2r[1]) + (b2r[2] + b2r[3])) + ((b2r[4] + b2r[5]) + b2r[6]), at_y, y)

    for stream, mine in enumerate((y, z, z, y)):
        arrived(p3r.at[stream], 8 + stream)
        total = p3[stream, mine]
        for k in range(7):
            total = total + p3r[stream, k]
        out_ref[stream] = total[:, 0:125] * (1.0 / 512.0)

    for swap in swaps:
        swap.wait_send()
    for channel, ref in enumerate((a1r, b1r, z1r, y1r, a2r, b2r, z2r, y2r)):
        departed(ref, channel)
    for stream in range(4):
        departed(p3r.at[stream], 8 + stream)


def local(correlators, momenta, source_channel, phase_code):
    f32, bf16 = jnp.float32, jnp.bfloat16
    vmem = pl.BlockSpec(memory_space=pltpu.VMEM)
    long = [(8, 4, 2, 8, 128), (7, 4, 2, 8, 128), (4, 2, 8, 128), (3, 2, 8, 128)]
    wide = [(4, 8, 2, 8, 128), (3, 8, 2, 8, 128), (8, 2, 8, 128), (7, 2, 8, 128)]
    scratch = [
        pltpu.VMEM((4, 4096, 128), bf16),
        pltpu.VMEM((3, 128), jnp.int32),
        pltpu.VMEM((1024, 256), bf16),
        pltpu.VMEM((512, 1024), bf16),
    ]
    scratch += [pltpu.VMEM((4, 8, 2, 32, 128), f32)] * 3
    scratch += [pltpu.VMEM(shape, f32) for shape in long + long + wide + wide]
    scratch += [pltpu.VMEM((4, 8, 2, 128), f32), pltpu.VMEM((4, 7, 2, 128), f32)]
    scratch += [pltpu.SemaphoreType.DMA((4,))] * 3 + [pltpu.SemaphoreType.DMA((12,))] * 2
    out = pl.pallas_call(
        kernel,
        out_shape=jax.ShapeDtypeStruct((4, 2, 125), f32),
        in_specs=[pl.BlockSpec(memory_space=pl.ANY), vmem, vmem, vmem],
        out_specs=vmem,
        scratch_shapes=scratch,
        compiler_params=pltpu.CompilerParams(collective_id=0, has_side_effects=True),
        name="project",
    )(
        correlators.reshape(-1, correlators.shape[-1]),
        momenta.T,
        source_channel.reshape(1, -1),
        phase_code.reshape(1, -1),
    )
    return jnp.transpose(out, (0, 2, 1))


def solution(mesh):
    return jax.shard_map(
        local,
        mesh=mesh,
        in_specs=(P(None, "gx", "gy", "gz", None), P(), P(), P()),
        out_specs=P("gx", None, ("gy", "gz")),
        check_vma=False,
    )
```

```python
import math

import jax
import jax.numpy as jnp
from jax import lax
from jax.experimental import pallas as pl
from jax.experimental.pallas import tpu as pltpu
from jax.sharding import PartitionSpec as P

MESH = pl.DeviceIdType.MESH
ORDER = (2, 1, 3, 0)
SLOT = {k: i for i, k in enumerate(ORDER)}
NT = (((1,), (1,)), ((), ()))


def phase_weights(mom_ref, padded, weights):
    padded[...] = jnp.zeros_like(padded)
    padded[:, 0:125] = mom_ref[...]
    own = lax.broadcasted_iota(jnp.int32, (8, 128), 0)
    cos, sin = [], []
    for row, axis in enumerate(("gx", "gy", "gz")):
        turns = (padded[row : row + 1, :] * (own + 8 * lax.axis_index(axis))) & 63
        angle = turns.astype(jnp.float32) * (2.0 * math.pi / 64.0)
        cos.append(jnp.cos(angle))
        sin.append(jnp.sin(angle))
    cos_yz = jnp.concatenate([cos[1][y : y + 1] * cos[2] - sin[1][y : y + 1] * sin[2] for y in range(8)], axis=0)
    sin_yz = jnp.concatenate([sin[1][y : y + 1] * cos[2] + cos[1][y : y + 1] * sin[2] for y in range(8)], axis=0)
    for x in range(8):
        c = (cos[0][x : x + 1] * cos_yz - sin[0][x : x + 1] * sin_yz).astype(jnp.bfloat16)
        s = (sin[0][x : x + 1] * cos_yz + cos[0][x : x + 1] * sin_yz).astype(jnp.bfloat16)
        rows, more = pl.ds(64 * x, 64), pl.ds(512 + 64 * x, 64)
        weights[rows, 0:128] = c
        weights[rows, 128:256] = -s
        weights[more, 0:128] = s
        weights[more, 128:256] = c


def mixing_rows(src_ref, code_ref, core):
    raw = lax.broadcasted_iota(jnp.int32, (128, 64), 0)
    src, code = src_ref[...], code_ref[...]
    one, none = jnp.float32(1.0), jnp.float32(0.0)
    real_sign = jnp.where(code == 0, one, jnp.where(code == 2, -one, none))
    imag_sign = jnp.where(code == 1, one, jnp.where(code == 3, -one, none))
    from_real = jnp.where(raw == src, one, none)
    from_imag = jnp.where(raw == src + 64, one, none)
    to_real = from_real * real_sign - from_imag * imag_sign
    to_imag = from_real * imag_sign + from_imag * real_sign
    row = lax.broadcasted_iota(jnp.int32, (64, 64), 0)
    channel = lax.broadcasted_iota(jnp.int32, (64, 64), 1)
    outer, inner, last = (row >> 3) & 3, (row >> 1) & 3, row & 1
    side = (row >> 5) ^ core
    result = []
    for z, y in ((outer, inner), (inner, outer)):
        chosen = jnp.where(channel == z * 16 + y * 4 + side * 2 + last, one, none).astype(jnp.bfloat16)
        parts = [
            lax.dot_general(chosen, part.astype(jnp.bfloat16), NT, preferred_element_type=jnp.float32)
            for part in (to_real, to_imag)
        ]
        result.append(jnp.concatenate(parts, axis=0).astype(jnp.bfloat16))
    return result


def kernel(corr, mom_hbm, src_hbm, code_hbm, out_ref, inbuf, mom_ref, src_ref, code_ref, padded, weights, left, own, give, take,
           z1, z1r, z2, z2r, y1, y1r, y2, y2r, a1, a1r, a2, a2r, b1, b1r, b2, b2r, p3, p3r,
           in_sem, small_sem, core_send, core_recv, send_sem, recv_sem):
    gx, gy, gz = lax.axis_index("gx"), lax.axis_index("gy"), lax.axis_index("gz")
    x, y_hi, z, y_lo, core = gx // 2, gx % 2, gy, gz // 2, gz % 2
    y = y_hi * 4 + y_lo

    def at_x(k):
        return (((x + k) % 4) * 2 + y_hi, gy, gz)

    def at_y(k):
        to = (y + k) % 8
        return ((x * 2 + to // 4), gy, (to % 4) * 2 + core)

    def at_z(k):
        return (gx, (z + k) % 8, gz)

    partner = (gx, gy, y_lo * 2 + (1 - core))

    barrier = pltpu.get_barrier_semaphore()
    peers = [partner] + [at_x(k) for k in range(1, 4)]
    peers += [at_y(k) for k in range(1, 8)] + [at_z(k) for k in range(1, 8)]
    for peer in peers:
        pl.semaphore_signal(barrier, inc=1, device_id=peer, device_id_type=MESH)

    loads = []
    for i, k in enumerate(ORDER):
        rows = pl.ds(pl.multiple_of(((x + k) % 4) * 4096, 4096), 4096)
        load = pltpu.make_async_copy(corr.at[rows], inbuf.at[i], in_sem.at[i])
        load.start()
        loads.append(load)
    small = []
    for i, (src, dst) in enumerate(((mom_hbm, mom_ref), (src_hbm, src_ref), (code_hbm, code_ref))):
        load = pltpu.make_async_copy(src, dst, small_sem.at[i])
        load.start()
        small.append(load)
    for load in small:
        load.wait()

    phase_weights(mom_ref, padded, weights)
    mix_zy, mix_yz = mixing_rows(src_ref, code_ref, core)

    sent = []

    def send(src, dst, channel, to):
        copy = pltpu.make_async_remote_copy(
            src_ref=src, dst_ref=dst, send_sem=send_sem.at[channel], recv_sem=recv_sem.at[channel],
            device_id=to, device_id_type=MESH)
        copy.start()

    def arrived(ref, channel):
        pltpu.make_async_copy(ref, ref, recv_sem.at[channel]).wait()

    def departed(ref, channel):
        pltpu.make_async_copy(ref, ref, send_sem.at[channel]).wait()

    swaps = []

    def compute(i):
        loads[i].wait()
        for t in range(8):
            mix = mix_zy if t % 4 in (0, 3) else mix_yz
            mixed = lax.dot_general(
                mix, inbuf[i, t * 512 : (t + 1) * 512, :], NT, preferred_element_type=jnp.float32
            ).astype(jnp.bfloat16)
            left[t * 64 : (t + 1) * 64, 0:512] = mixed[0:64]
            left[t * 64 : (t + 1) * 64, 512:1024] = mixed[64:128]
        product = jnp.dot(left[...], weights[...], preferred_element_type=jnp.float32)
        for t in range(8):
            for half in range(2):
                lanes = slice(half * 128, half * 128 + 128)
                own[i, t, half] = product[t * 64 : t * 64 + 32, lanes]
                give[i, t, half] = product[t * 64 + 32 : t * 64 + 64, lanes]
        if i == 0:
            pl.semaphore_wait(barrier, len(peers))
        swap = pltpu.make_async_remote_copy(
            src_ref=give.at[i], dst_ref=take.at[i], send_sem=core_send.at[i], recv_sem=core_recv.at[i],
            device_id=partner, device_id_type=MESH)
        swap.start()
        swaps.append(swap)

    def first_phase(i):
        swaps[i].wait_recv()
        for yh in range(2):
            for half in range(2):
                for tt in range(4):
                    t = yh * 4 + tt
                    value = (own[i, t, half] + take[i, t, half]).reshape(4, 8, 128)
                    if tt == 0:
                        for q in range(4):
                            z1[half * 4 + q, i, yh] = value[q]
                    elif tt == 1:
                        for q in range(4):
                            y1[yh * 4 + q, i, half] = value[q]
                    elif tt == 2:
                        for q in range(4):
                            a1[i, yh * 4 + q, half] = value[q]
                    else:
                        for q in range(4):
                            b1[i, half * 4 + q, yh] = value[q]
        k = ORDER[i]
        if k != 0:
            send(a1.at[i], a1r.at[k - 1], 0, at_x(k))
            send(b1.at[i], b1r.at[k - 1], 1, at_x(k))
        for k in (4, 3, 5, 2, 6, 1, 7):
            send(z1.at[(z + k) % 8, i], z1r.at[k - 1, i], 2, at_z(k))
            send(y1.at[(y + k) % 8, i], y1r.at[k - 1, i], 3, at_y(k))

    for i in range(4):
        compute(i)
        if i >= 1:
            first_phase(i - 1)
    first_phase(3)

    arrived(a1r, 0)
    a2[...] = a1[SLOT[0]] + a1r[0] + a1r[1] + a1r[2]
    for k in (4, 3, 5, 2, 6, 1, 7):
        send(a2.at[(y + k) % 8], a2r.at[k - 1], 4, at_y(k))
    arrived(b1r, 1)
    b2[...] = b1[SLOT[0]] + b1r[0] + b1r[1] + b1r[2]
    for k in (4, 3, 5, 2, 6, 1, 7):
        send(b2.at[(z + k) % 8], b2r.at[k - 1], 5, at_z(k))
    arrived(z1r, 2)
    z2[...] = z1[z] + ((z1r[0] + z1r[1]) + (z1r[2] + z1r[3])) + ((z1r[4] + z1r[5]) + z1r[6])
    for k in (2, 1, 3):
        send(z2.at[SLOT[k]], z2r.at[k - 1], 6, at_x(k))
    arrived(y1r, 3)
    y2[...] = y1[y] + ((y1r[0] + y1r[1]) + (y1r[2] + y1r[3])) + ((y1r[4] + y1r[5]) + y1r[6])
    for k in (2, 1, 3):
        send(y2.at[SLOT[k]], y2r.at[k - 1], 7, at_x(k))

    def spread(stream, value, at, mine):
        rows = value.reshape(16, 128)
        for q in range(8):
            p3[stream, q] = rows[2 * q : 2 * q + 2]
        for k in (4, 3, 5, 2, 6, 1, 7):
            send(p3.at[stream, (mine + k) % 8], p3r.at[stream, k - 1], 8 + stream, at(k))

    arrived(z2r, 6)
    spread(0, z2[SLOT[0]] + z2r[0] + z2r[1] + z2r[2], at_y, y)
    arrived(y2r, 7)
    spread(1, y2[SLOT[0]] + y2r[0] + y2r[1] + y2r[2], at_z, z)
    arrived(a2r, 4)
    spread(2, a2[y] + ((a2r[0] + a2r[1]) + (a2r[2] + a2r[3])) + ((a2r[4] + a2r[5]) + a2r[6]), at_z, z)
    arrived(b2r, 5)
    spread(3, b2[z] + ((b2r[0] + b2r[1]) + (b2r[2] + b2r[3])) + ((b2r[4] + b2r[5]) + b2r[6]), at_y, y)

    for stream, mine in enumerate((y, z, z, y)):
        arrived(p3r.at[stream], 8 + stream)
        total = p3[stream, mine]
        for k in range(7):
            total = total + p3r[stream, k]
        out_ref[stream] = total[:, 0:125] * (1.0 / 512.0)

    for swap in swaps:
        swap.wait_send()
    for channel, ref in enumerate((a1r, b1r, z1r, y1r, a2r, b2r, z2r, y2r)):
        departed(ref, channel)
    for stream in range(4):
        departed(p3r.at[stream], 8 + stream)


def local(correlators, momenta, source_channel, phase_code):
    f32, bf16 = jnp.float32, jnp.bfloat16
    hbm = pl.BlockSpec(memory_space=pltpu.HBM)
    long = [(8, 4, 2, 8, 128), (7, 4, 2, 8, 128), (4, 2, 8, 128), (3, 2, 8, 128)]
    wide = [(4, 8, 2, 8, 128), (3, 8, 2, 8, 128), (8, 2, 8, 128), (7, 2, 8, 128)]
    scratch = [
        pltpu.VMEM((4, 4096, 128), bf16),
        pltpu.VMEM((3, 125), jnp.int32),
        pltpu.VMEM((1, 64), jnp.int32),
        pltpu.VMEM((1, 64), jnp.int32),
        pltpu.VMEM((3, 128), jnp.int32),
        pltpu.VMEM((1024, 256), bf16),
        pltpu.VMEM((512, 1024), bf16),
    ]
    scratch += [pltpu.VMEM((4, 8, 2, 32, 128), f32)] * 3
    scratch += [pltpu.VMEM(shape, f32) for shape in long + long + wide + wide]
    scratch += [pltpu.VMEM((4, 8, 2, 128), f32), pltpu.VMEM((4, 7, 2, 128), f32)]
    scratch += [pltpu.SemaphoreType.DMA((4,)), pltpu.SemaphoreType.DMA((3,))] + [pltpu.SemaphoreType.DMA((4,))] * 2 + [pltpu.SemaphoreType.DMA((12,))] * 2
    out = pl.pallas_call(
        kernel,
        out_shape=jax.ShapeDtypeStruct((4, 2, 125), f32),
        in_specs=[hbm, hbm, hbm, hbm],
        out_specs=pl.BlockSpec(memory_space=pltpu.VMEM),
        scratch_shapes=scratch,
        compiler_params=pltpu.CompilerParams(collective_id=0, has_side_effects=True, vmem_limit_bytes=24 * 1024 * 1024),
        name="project",
    )(
        *(
            pltpu.with_memory_space_constraint(value, pltpu.HBM)
            for value in (
                correlators.reshape(-1, correlators.shape[-1]),
                momenta.T,
                source_channel.reshape(1, -1),
                phase_code.reshape(1, -1),
            )
        )
    )
    return jnp.transpose(out, (0, 2, 1))


def solution(mesh):
    return jax.shard_map(
        local,
        mesh=mesh,
        in_specs=(P(None, "gx", "gy", "gz", None), P(), P(), P()),
        out_specs=P("gx", None, ("gy", "gz")),
        check_vma=False,
    )
```

```python
import math

import jax
import jax.numpy as jnp
from jax import lax
from jax.experimental import pallas as pl
from jax.experimental.pallas import tpu as pltpu
from jax.sharding import PartitionSpec as P

MESH = pl.DeviceIdType.MESH
ORDER = (2, 1, 3, 0)
SLOT = {k: i for i, k in enumerate(ORDER)}
FAR_FIRST = (4, 3, 5, 2, 6, 1, 7)
NT = (((1,), (1,)), ((), ()))


def phase_weights(mom_ref, padded, weights):
    padded[...] = jnp.zeros_like(padded)
    padded[:, 0:125] = mom_ref[...]
    own = lax.broadcasted_iota(jnp.int32, (8, 128), 0)
    cos, sin = [], []
    for row, axis in enumerate(("gx", "gy", "gz")):
        turns = (padded[row : row + 1, :] * (own + 8 * lax.axis_index(axis))) & 63
        angle = turns.astype(jnp.float32) * (2.0 * math.pi / 64.0)
        cos.append(jnp.cos(angle))
        sin.append(jnp.sin(angle))
    cos_yz = jnp.concatenate([cos[1][y : y + 1] * cos[2] - sin[1][y : y + 1] * sin[2] for y in range(8)], axis=0)
    sin_yz = jnp.concatenate([sin[1][y : y + 1] * cos[2] + cos[1][y : y + 1] * sin[2] for y in range(8)], axis=0)
    for x in range(8):
        c = (cos[0][x : x + 1] * cos_yz - sin[0][x : x + 1] * sin_yz).astype(jnp.bfloat16)
        s = (sin[0][x : x + 1] * cos_yz + cos[0][x : x + 1] * sin_yz).astype(jnp.bfloat16)
        rows, more = pl.ds(64 * x, 64), pl.ds(512 + 64 * x, 64)
        weights[rows, 0:128] = c
        weights[rows, 128:256] = -s
        weights[more, 0:128] = s
        weights[more, 128:256] = c


def mixing_rows(src_ref, code_ref, core):
    raw = lax.broadcasted_iota(jnp.int32, (128, 64), 0)
    src, code = src_ref[...], code_ref[...]
    one, none = jnp.float32(1.0), jnp.float32(0.0)
    real_sign = jnp.where(code == 0, one, jnp.where(code == 2, -one, none))
    imag_sign = jnp.where(code == 1, one, jnp.where(code == 3, -one, none))
    from_real = jnp.where(raw == src, one, none)
    from_imag = jnp.where(raw == src + 64, one, none)
    to_real = from_real * real_sign - from_imag * imag_sign
    to_imag = from_real * imag_sign + from_imag * real_sign
    row = lax.broadcasted_iota(jnp.int32, (64, 64), 0)
    channel = lax.broadcasted_iota(jnp.int32, (64, 64), 1)
    outer, inner, last = (row >> 3) & 3, (row >> 1) & 3, row & 1
    side = (row >> 5) ^ core
    result = []
    for z, y in ((outer, inner), (inner, outer)):
        chosen = jnp.where(channel == z * 16 + y * 4 + side * 2 + last, one, none).astype(jnp.bfloat16)
        parts = [
            lax.dot_general(chosen, part.astype(jnp.bfloat16), NT, preferred_element_type=jnp.float32)
            for part in (to_real, to_imag)
        ]
        result.append(jnp.concatenate(parts, axis=0).astype(jnp.bfloat16))
    return result


def kernel(corr, mom_hbm, src_hbm, code_hbm, out_ref, inbuf, mom_ref, src_ref, code_ref, padded, weights, left, own, give, take,
           z1, z1r, z2, z2r, y1, y1r, y2, y2r, a1, a1r, a2, a2r, b1, b1r, b2, b2r, p3, p3r,
           in_sem, small_sem, core_send, core_recv, send_sem, recv_sem):
    gx, gy, gz = lax.axis_index("gx"), lax.axis_index("gy"), lax.axis_index("gz")
    x, y_hi, z, y_lo, core = gx // 2, gx % 2, gy, gz // 2, gz % 2
    y = y_hi * 4 + y_lo

    def at_x(k):
        return (((x + k) % 4) * 2 + y_hi, gy, gz)

    def at_y(k):
        to = (y + k) % 8
        return ((x * 2 + to // 4), gy, (to % 4) * 2 + core)

    def at_z(k):
        return (gx, (z + k) % 8, gz)

    partner = (gx, gy, y_lo * 2 + (1 - core))

    barrier = pltpu.get_barrier_semaphore()
    peers = [partner] + [at_x(k) for k in range(1, 4)]
    peers += [at_y(k) for k in range(1, 8)] + [at_z(k) for k in range(1, 8)]
    for peer in peers:
        pl.semaphore_signal(barrier, inc=1, device_id=peer, device_id_type=MESH)

    loads = []
    for i, k in enumerate(ORDER):
        rows = pl.ds(pl.multiple_of(((x + k) % 4) * 4096, 4096), 4096)
        load = pltpu.make_async_copy(corr.at[rows], inbuf.at[i], in_sem.at[i])
        load.start()
        loads.append(load)
    small = []
    for i, (src, dst) in enumerate(((mom_hbm, mom_ref), (src_hbm, src_ref), (code_hbm, code_ref))):
        load = pltpu.make_async_copy(src, dst, small_sem.at[i])
        load.start()
        small.append(load)
    for load in small:
        load.wait()

    phase_weights(mom_ref, padded, weights)
    mix_zy, mix_yz = mixing_rows(src_ref, code_ref, core)

    sent = []

    def send(src, dst, channel, to):
        copy = pltpu.make_async_remote_copy(
            src_ref=src, dst_ref=dst, send_sem=send_sem.at[channel], recv_sem=recv_sem.at[channel],
            device_id=to, device_id_type=MESH)
        copy.start()

    def arrived(ref, channel):
        pltpu.make_async_copy(ref, ref, recv_sem.at[channel]).wait()

    def departed(ref, channel):
        pltpu.make_async_copy(ref, ref, send_sem.at[channel]).wait()

    swaps = {}

    def compute(i):
        loads[i].wait()
        for t in range(8):
            mix = mix_zy if t % 4 in (0, 3) else mix_yz
            mixed = lax.dot_general(
                mix, inbuf[i, t * 512 : (t + 1) * 512, :], NT, preferred_element_type=jnp.float32
            ).astype(jnp.bfloat16)
            left[t * 64 : (t + 1) * 64, 0:512] = mixed[0:64]
            left[t * 64 : (t + 1) * 64, 512:1024] = mixed[64:128]
        product = jnp.dot(left[...], weights[...], preferred_element_type=jnp.float32)
        for t in range(8):
            for half in range(2):
                lanes = slice(half * 128, half * 128 + 128)
                at = (i, t % 4 // 2, t // 4 * 2 + t % 2, half)
                own[at] = product[t * 64 : t * 64 + 32, lanes]
                give[at] = product[t * 64 + 32 : t * 64 + 64, lanes]
        if i == 0:
            pl.semaphore_wait(barrier, len(peers))
        for part in (1, 0):
            swap = pltpu.make_async_remote_copy(
                src_ref=give.at[i, part], dst_ref=take.at[i, part], send_sem=core_send.at[2 * i + part],
                recv_sem=core_recv.at[2 * i + part], device_id=partner, device_id_type=MESH)
            swap.start()
            swaps[i, part] = swap

    def first_phase(i):
        def sums(part):
            swaps[i, part].wait_recv()
            for yh in range(2):
                for half in range(2):
                    for j in range(2):
                        at = (i, part, yh * 2 + j, half)
                        yield yh, half, j, (own[at] + take[at]).reshape(4, 8, 128)

        for yh, half, j, value in sums(1):
            for q in range(4):
                if j == 0:
                    a1[i, half, yh * 4 + q] = value[q]
                else:
                    b1[i, yh, half * 4 + q] = value[q]
        k = ORDER[i]
        if k != 0:
            for piece in range(2):
                send(a1.at[i, piece], a1r.at[k - 1, piece], piece, at_x(k))
                send(b1.at[i, piece], b1r.at[k - 1, piece], 2 + piece, at_x(k))
        for yh, half, j, value in sums(0):
            for q in range(4):
                if j == 0:
                    z1[half * 4 + q, i, yh] = value[q]
                else:
                    y1[yh * 4 + q, i, half] = value[q]
        for k in FAR_FIRST:
            send(z1.at[(z + k) % 8, i], z1r.at[k - 1, i], 4, at_z(k))
            send(y1.at[(y + k) % 8, i], y1r.at[k - 1, i], 5, at_y(k))

    for i in range(4):
        compute(i)
        if i >= 1:
            first_phase(i - 1)
    first_phase(3)

    for piece in range(2):
        arrived(a1r.at[:, piece], piece)
        a2[piece] = a1[SLOT[0], piece] + a1r[0, piece] + a1r[1, piece] + a1r[2, piece]
        for k in FAR_FIRST:
            send(a2.at[piece, (y + k) % 8], a2r.at[piece, k - 1], 6, at_y(k))
        arrived(b1r.at[:, piece], 2 + piece)
        b2[piece] = b1[SLOT[0], piece] + b1r[0, piece] + b1r[1, piece] + b1r[2, piece]
        for k in FAR_FIRST:
            send(b2.at[piece, (z + k) % 8], b2r.at[piece, k - 1], 7, at_z(k))
    arrived(z1r, 4)
    z2[...] = z1[z] + ((z1r[0] + z1r[1]) + (z1r[2] + z1r[3])) + ((z1r[4] + z1r[5]) + z1r[6])
    for k in (2, 1, 3):
        send(z2.at[SLOT[k]], z2r.at[k - 1], 8, at_x(k))
    arrived(y1r, 5)
    y2[...] = y1[y] + ((y1r[0] + y1r[1]) + (y1r[2] + y1r[3])) + ((y1r[4] + y1r[5]) + y1r[6])
    for k in (2, 1, 3):
        send(y2.at[SLOT[k]], y2r.at[k - 1], 9, at_x(k))

    def spread(stream, value, at, mine):
        rows = value.reshape(16, 128)
        for q in range(8):
            p3[stream, q] = rows[2 * q : 2 * q + 2]
        for k in FAR_FIRST:
            send(p3.at[stream, (mine + k) % 8], p3r.at[stream, k - 1], 10 + stream, at(k))

    def all_of(mine, other):
        total = mine
        for k in range(7):
            total = total + other[:, k]
        return total

    arrived(z2r, 8)
    spread(0, z2[SLOT[0]] + z2r[0] + z2r[1] + z2r[2], at_y, y)
    arrived(y2r, 9)
    spread(1, y2[SLOT[0]] + y2r[0] + y2r[1] + y2r[2], at_z, z)
    arrived(a2r, 6)
    spread(2, all_of(a2[:, y], a2r), at_z, z)
    arrived(b2r, 7)
    spread(3, all_of(b2[:, z], b2r), at_y, y)

    for stream, mine in enumerate((y, z, z, y)):
        arrived(p3r.at[stream], 10 + stream)
        total = p3[stream, mine]
        for k in range(7):
            total = total + p3r[stream, k]
        out_ref[stream] = total[:, 0:125] * (1.0 / 512.0)

    for swap in swaps.values():
        swap.wait_send()
    for piece in range(2):
        departed(a1r.at[:, piece], piece)
        departed(b1r.at[:, piece], 2 + piece)
    for channel, ref in enumerate((z1r, y1r, a2r, b2r, z2r, y2r)):
        departed(ref, 4 + channel)
    for stream in range(4):
        departed(p3r.at[stream], 10 + stream)


def local(correlators, momenta, source_channel, phase_code):
    f32, bf16 = jnp.float32, jnp.bfloat16
    hbm = pl.BlockSpec(memory_space=pltpu.HBM)
    long = [(8, 4, 2, 8, 128), (7, 4, 2, 8, 128), (4, 2, 8, 128), (3, 2, 8, 128)]
    wide = [(4, 2, 8, 8, 128), (3, 2, 8, 8, 128), (2, 8, 8, 128), (2, 7, 8, 128)]
    scratch = [
        pltpu.VMEM((4, 4096, 128), bf16),
        pltpu.VMEM((3, 125), jnp.int32),
        pltpu.VMEM((1, 64), jnp.int32),
        pltpu.VMEM((1, 64), jnp.int32),
        pltpu.VMEM((3, 128), jnp.int32),
        pltpu.VMEM((1024, 256), bf16),
        pltpu.VMEM((512, 1024), bf16),
    ]
    scratch += [pltpu.VMEM((4, 2, 4, 2, 32, 128), f32)] * 3
    scratch += [pltpu.VMEM(shape, f32) for shape in long + long + wide + wide]
    scratch += [pltpu.VMEM((4, 8, 2, 128), f32), pltpu.VMEM((4, 7, 2, 128), f32)]
    scratch += [pltpu.SemaphoreType.DMA((4,)), pltpu.SemaphoreType.DMA((3,))] + [pltpu.SemaphoreType.DMA((8,))] * 2 + [pltpu.SemaphoreType.DMA((14,))] * 2
    out = pl.pallas_call(
        kernel,
        out_shape=jax.ShapeDtypeStruct((4, 2, 125), f32),
        in_specs=[hbm, hbm, hbm, hbm],
        out_specs=pl.BlockSpec(memory_space=pltpu.VMEM),
        scratch_shapes=scratch,
        compiler_params=pltpu.CompilerParams(collective_id=0, has_side_effects=True, vmem_limit_bytes=24 * 1024 * 1024),
        name="project",
    )(
        *(
            pltpu.with_memory_space_constraint(value, pltpu.HBM)
            for value in (
                correlators.reshape(-1, correlators.shape[-1]),
                momenta.T,
                source_channel.reshape(1, -1),
                phase_code.reshape(1, -1),
            )
        )
    )
    return jnp.transpose(out, (0, 2, 1))


def solution(mesh):
    return jax.shard_map(
        local,
        mesh=mesh,
        in_specs=(P(None, "gx", "gy", "gz", None), P(), P(), P()),
        out_specs=P("gx", None, ("gy", "gz")),
        check_vma=False,
    )
```
